16 devices in a mesh: dp: 2 (over y, z), sp: 8 (over x, core).
Axes of the slice: x: 4, y: 2, z: 1, core: 2. Of those that a mesh axis runs over, the one named last changes fastest.
The devices are a block of a 4x4x4 slice.
Arguments:
- x: bfloat16 [4096, 9216], P(('dp', 'sp')), parts along dimension 0
- gain: bfloat16 [9216], replicated
- wq: bfloat16 [9216, 9216], replicated
- wk: bfloat16 [9216, 9216], replicated
- wv: bfloat16 [9216, 9216], replicated
- wo: bfloat16 [9216, 9216], replicated
Outputs:
- output: bfloat16 [4096, 9216], P(('dp', 'sp')), parts along dimension 0
There are 2 independent parts. The reference program is written for one: setup_inputs(seed, part) draws one part's arguments, and reference() takes and returns one part's arrays. A program takes and returns all parts, laid end to end along the dimension named above; an argument that names none is the same for every part.
All inputs are finite; a program needn't handle non-finite values.
Results may differ from the reference program's by a relative error of at most 0.012.
Values are sent between devices in bfloat16 or wider.
A program may use at most 1.5 GiB of HBM per device.

```python
import jax
import jax.numpy as jnp
from jax import lax

ROWS = 2048
D = 9216
HEADS = 72
KV_HEADS = 72
HEAD = 128
THETA = 10000


def setup_inputs(seed: int = 0, part: int = 0) -> dict:
    kx, kn, kq, kk, kv, ko = jax.random.split(jax.random.key(seed), 6)

    def weights(key, rows, columns):
        return jax.random.normal(key, (rows, columns), jnp.float32) * rows**-0.5

    drawn = {
        "x": jax.random.normal(jax.random.fold_in(kx, part), (ROWS, D), jnp.float32),
        "gain": 1 + 0.1 * jax.random.normal(kn, (D,), jnp.float32),
        "wq": 2 * weights(kq, D, HEADS * HEAD),
        "wk": 2 * weights(kk, D, KV_HEADS * HEAD),
        "wv": 4 * weights(kv, D, KV_HEADS * HEAD),
        "wo": weights(ko, HEADS * HEAD, D),
    }
    return {k: v.astype(jnp.bfloat16) for k, v in drawn.items()}


def normed(x, gain):
    wide = x.astype(jnp.float32)
    scale = lax.rsqrt(jnp.mean(wide * wide, -1, keepdims=True) + 1e-6)
    return (wide * scale * gain.astype(jnp.float32)).astype(jnp.bfloat16)


def turned(t, place, theta):
    half = t.shape[-1] // 2
    angle = place.astype(jnp.float32)[:, None] * theta ** (-jnp.arange(half, dtype=jnp.float32) / half)
    cos, sin = jnp.cos(angle)[:, None], jnp.sin(angle)[:, None]
    a, b = t[..., :half].astype(jnp.float32), t[..., half:].astype(jnp.float32)
    return jnp.concatenate([a * cos - b * sin, b * cos + a * sin], -1).astype(jnp.bfloat16)


def matmul(a, w):
    return jnp.dot(a, w, preferred_element_type=jnp.float32).astype(jnp.bfloat16)


def einsum(form, a, b):
    return jnp.einsum(form, a.astype(jnp.float32), b.astype(jnp.float32))


def attention(q, k, v):
    scores = einsum("tgsd,ugd->gstu", q, k) * q.shape[-1] ** -0.5
    token = jnp.arange(q.shape[0])
    scores = jnp.where(token[:, None] >= token, scores, -jnp.inf)
    weights = jax.nn.softmax(scores, -1).astype(jnp.bfloat16)
    return einsum("gstu,ugd->tgsd", weights, v).astype(jnp.bfloat16)


def reference(x, gain, wq, wk, wv, wo):
    a, place = normed(x, gain), jnp.arange(ROWS)
    q = turned(matmul(a, wq).reshape(ROWS, HEADS, HEAD), place, THETA).reshape(ROWS, KV_HEADS, -1, HEAD)
    k = turned(matmul(a, wk).reshape(ROWS, KV_HEADS, HEAD), place, THETA)
    v = matmul(a, wv).reshape(ROWS, KV_HEADS, HEAD)
    seen = attention(q, k, v).reshape(ROWS, HEADS * HEAD)
    return (x.astype(jnp.float32) + jnp.dot(seen, wo, preferred_element_type=jnp.float32)).astype(jnp.bfloat16)
```

```python
import functools

import jax
import jax.numpy as jnp
from jax import lax
from jax.experimental import pallas as pl
from jax.experimental.pallas import tpu as pltpu
from jax.sharding import PartitionSpec as P

NEG = -1e30
HIDDEN = 2 * NEG
LOG2E = 1.4426950408889634
HEAD = 128
THETA = 10000
MESH = pl.DeviceIdType.MESH
VMEM = 63 * 2**20

TILE_HEADS = 4
W_SLOTS = 4
S_SLOTS = 12
STRIDE = 7
OUT_TILE = 1024
O_SLOTS = 4
BK = 512


def _dot(a, b, ca=1, cb=0):
    return lax.dot_general(a, b, (((ca,), (cb,)), ((), ())), preferred_element_type=jnp.float32)


def _greet(n):
    me = lax.axis_index("sp")
    barrier = pltpu.get_barrier_semaphore()
    for d in range(1, n):
        pl.semaphore_signal(barrier, inc=1, device_id={"sp": lax.rem(me + d, n)}, device_id_type=MESH)
    pl.semaphore_wait(barrier, n - 1)


def _project(n, x_ref, gain_ref, cos_ref, sin_ref, wq_ref, wk_ref, wv_ref, o_ref, a_s, w_s, acc_s, out_s, w_sem, s_sem, r_sem):
    me = lax.axis_index("sp")
    own, width = x_ref.shape
    per = o_ref.shape[1]
    cols = TILE_HEADS * HEAD
    tiles = wq_ref.shape[1] // cols
    steps = 3 * tiles
    weights = (wq_ref, wk_ref, wv_ref)
    offset = lax.div(me * per, TILE_HEADS)

    def tile_of(t):
        return lax.rem(STRIDE * lax.rem(t, tiles) + offset, tiles)

    def fetch(t):
        slot = lax.rem(t, W_SLOTS)
        at = pl.multiple_of(tile_of(t) * cols, cols)
        for m, w in enumerate(weights):
            @pl.when(lax.div(t, tiles) == m)
            def _():
                pltpu.make_async_copy(w.at[:, pl.ds(at, cols)], w_s.at[slot], w_sem.at[slot]).start()

    def fetched(t):
        slot = lax.rem(t, W_SLOTS)
        pltpu.make_async_copy(wq_ref.at[:, pl.ds(0, cols)], w_s.at[slot], w_sem.at[slot]).wait()

    def send(t):
        slot, m = lax.rem(t, S_SLOTS), lax.div(t, tiles)
        first = tile_of(t) * TILE_HEADS
        for h in range(TILE_HEADS):
            to, local = lax.div(first + h, per), lax.rem(first + h, per)
            src = out_s.at[slot, h]
            dst = o_ref.at[m, local, pl.ds(me * own, own), :]

            @pl.when(to == me)
            def _():
                pltpu.make_async_copy(src, dst, s_sem.at[slot, h]).start()

            @pl.when(to != me)
            def _():
                pltpu.make_async_remote_copy(src_ref=src, dst_ref=dst, send_sem=s_sem.at[slot, h], recv_sem=r_sem.at[me],
                                             device_id={"sp": to}, device_id_type=MESH).start()

    def sent(t):
        slot = lax.rem(t, S_SLOTS)
        for h in range(TILE_HEADS):
            pltpu.make_async_copy(out_s.at[slot, h], o_ref.at[0, 0, pl.ds(0, own), :], s_sem.at[slot, h]).wait()

    def finish(t):
        prev, slot = lax.rem(t, 2), lax.rem(t, S_SLOTS)
        plain = lax.div(t, tiles) == 2
        for h in range(TILE_HEADS):
            b = acc_s[prev, :, h * HEAD : (h + 1) * HEAD].astype(jnp.bfloat16).astype(jnp.float32)
            turned = b * cos_ref[...] + pltpu.roll(b, HEAD // 2, 1) * sin_ref[...]
            out_s[slot, h] = jnp.where(plain, b, turned).astype(jnp.bfloat16)

    def multiply(t):
        acc_s[lax.rem(t, 2)] = _dot(a_s[...], w_s[lax.rem(t, W_SLOTS)])

    for t in range(W_SLOTS - 1):
        fetch(t)

    def norm(i, _):
        rows = pl.ds(i * 16, 16)
        wide = x_ref[rows, :].astype(jnp.float32)
        scale = lax.rsqrt(jnp.sum(wide * wide, -1, keepdims=True) * (1 / width) + 1e-6)
        a_s[rows, :] = (wide * scale * gain_ref[...].astype(jnp.float32)).astype(jnp.bfloat16)

    lax.fori_loop(0, own // 16, norm, None)
    _greet(n)
    fetched(0)
    fetch(W_SLOTS - 1)
    multiply(0)

    def step(t, _):
        @pl.when(t + W_SLOTS - 1 < steps)
        def _():
            fetch(t + W_SLOTS - 1)

        @pl.when(t >= 2)
        def _():
            send(t - 2)

        @pl.when(t - 1 >= S_SLOTS)
        def _():
            sent(t - 1 - S_SLOTS)

        fetched(t)
        finish(t - 1)
        multiply(t)

    lax.fori_loop(1, steps, step, None)
    send(steps - 2)
    sent(steps - 1 - S_SLOTS)
    finish(steps - 1)
    send(steps - 1)
    lax.fori_loop(steps - S_SLOTS, steps, lambda t, _: sent(t), None)
    for d in range(1, n):
        src = lax.rem(me + d, n)
        block = o_ref.at[:, :, pl.ds(src * own, own), :]
        pltpu.make_async_copy(block, block, r_sem.at[src]).wait()


def project(n, x, gain, cos, sin, wq, wk, wv):
    own, width = x.shape
    per = wq.shape[1] // HEAD // n
    cols = TILE_HEADS * HEAD
    vm, hbm = pl.BlockSpec(memory_space=pltpu.VMEM), pl.BlockSpec(memory_space=pl.ANY)
    return pl.pallas_call(
        functools.partial(_project, n),
        out_shape=jax.ShapeDtypeStruct((3, per, n * own, HEAD), jnp.bfloat16),
        in_specs=[vm, vm, vm, vm, hbm, hbm, hbm],
        out_specs=hbm,
        scratch_shapes=[
            pltpu.VMEM((own, width), jnp.bfloat16),
            pltpu.VMEM((W_SLOTS, width, cols), jnp.bfloat16),
            pltpu.VMEM((2, own, cols), jnp.float32),
            pltpu.VMEM((S_SLOTS, TILE_HEADS, own, HEAD), jnp.bfloat16),
            pltpu.SemaphoreType.DMA((W_SLOTS,)),
            pltpu.SemaphoreType.DMA((S_SLOTS, TILE_HEADS)),
            pltpu.SemaphoreType.DMA((n,)),
        ],
        compiler_params=pltpu.CompilerParams(collective_id=0, has_side_effects=True, vmem_limit_bytes=VMEM),
        name="project",
    )(x, gain, cos, sin, wq, wk, wv)


def _pick(j, order):
    out = jnp.int32(order[0])
    for i, o in enumerate(order[1:], 1):
        out = jnp.where(j == i, o, out)
    return out


def _attend(n, order, qkv_ref, x_ref, wo_ref, y_ref, qkv_s, got_s, acc_s, w_s, top_s, mix_s, x_s, y_s,
            in_sem, w_sem, s_sem, r_sem, x_sem, y_sem):
    me = lax.axis_index("sp")
    chip, chips = lax.div(me, 2), n // 2
    heads, own = qkv_ref.shape[1], x_ref.shape[0]
    width = wo_ref.shape[1]
    tiles = width // OUT_TILE
    depth = 2 * heads * HEAD
    arrive = [0, 2, 1, 3] if chips == 4 else list(range(chips))
    steps = chips * tiles
    e = HEAD**-0.5 * LOG2E

    load = pltpu.make_async_copy(qkv_ref, qkv_s, in_sem)
    load.start()

    def source(i):
        return lax.rem(chip + _pick(i, arrive), chips)

    def w_copy(t):
        slot = lax.rem(t, O_SLOTS)
        row = pl.multiple_of(source(lax.div(t, tiles)) * depth, depth)
        col = pl.multiple_of(lax.rem(t, tiles) * OUT_TILE, OUT_TILE)
        return pltpu.make_async_copy(wo_ref.at[pl.ds(row, depth), pl.ds(col, OUT_TILE)], w_s.at[slot], w_sem.at[slot])

    for t in range(O_SLOTS - 1):
        w_copy(t).start()
    _greet(n)
    load.wait()

    ones = jnp.ones((8, BK), jnp.bfloat16)

    def send(j, iq):
        return pltpu.make_async_remote_copy(
            src_ref=qkv_s.at[0, :, pl.ds(iq * own, own), :], dst_ref=got_s.at[pl.ds(me * heads, heads)],
            send_sem=s_sem.at[j], recv_sem=r_sem.at[me], device_id={"sp": iq}, device_id_type=MESH)

    def queries(j, _):
        iq = lax.rem(me + _pick(j, order), n)
        rows = pl.ds(pl.multiple_of(iq * own, own), own)
        top_s[...] = jnp.full(top_s.shape, NEG, jnp.float32)
        mix_s[...] = jnp.zeros(mix_s.shape, jnp.float32)

        def block(first, bk, masked):
            here = pl.ds(pl.multiple_of(first, bk), bk)
            scores = [_dot(qkv_s[1, i, here, :], qkv_s[0, i, rows, :], 1, 1) for i in range(heads)]
            if masked:
                ok = lax.broadcasted_iota(jnp.int32, (bk, own), 1) >= lax.broadcasted_iota(jnp.int32, (bk, own), 0)
            weights, keeps = [], []
            for i, s in enumerate(scores):
                if masked:
                    s = jnp.where(ok, s, HIDDEN)
                old = top_s[i : i + 1, :]
                top = jnp.maximum(old, s.max(axis=0, keepdims=True))
                top_s[i : i + 1, :] = top
                weights.append(jnp.exp2((s - top) * e).astype(jnp.bfloat16))
                keeps.append(jnp.exp2((old - top) * e))
            for i, (p, keep) in enumerate(zip(weights, keeps)):
                values = jnp.concatenate([qkv_s[2, i, here, :].T, ones[:, :bk]], axis=0)
                mix_s[i] = mix_s[i] * keep + _dot(values, p)

        whole = lax.div(iq * own, BK)
        lax.fori_loop(0, whole, lambda b, _: block(b * BK, BK, False), None)
        lax.fori_loop(whole * (BK // own), iq, lambda b, _: block(b * own, own, False), None)
        block(iq * own, own, True)

        def result(i):
            total = mix_s[i, HEAD : HEAD + 1, :]
            return (mix_s[i, :HEAD, :] * (1 / total)).T.astype(jnp.bfloat16)

        @pl.when(j < n - 1)
        def _():
            for i in range(heads):
                qkv_s[0, i, rows, :] = result(i)
            send(j, iq).start()

        @pl.when(j == n - 1)
        def _():
            for i in range(heads):
                got_s[me * heads + i] = result(i)

    lax.fori_loop(0, n, queries, None)

    def x_copy(k):
        return pltpu.make_async_copy(x_ref.at[:, pl.ds(pl.multiple_of(k * OUT_TILE, OUT_TILE), OUT_TILE)], x_s.at[lax.rem(k, 2)], x_sem.at[lax.rem(k, 2)])

    def y_copy(k):
        return pltpu.make_async_copy(y_s.at[lax.rem(k, 2)], y_ref.at[:, pl.ds(pl.multiple_of(k * OUT_TILE, OUT_TILE), OUT_TILE)], y_sem.at[lax.rem(k, 2)])

    for c in range(chips):
        at = source(c)
        for core in range(2):
            src = at * 2 + core

            def arrived():
                block = got_s.at[pl.ds(src * heads, heads)]
                pltpu.make_async_copy(block, block, r_sem.at[src]).wait()

            if c == 0:
                pl.when(src != me)(arrived)
            else:
                arrived()
        last = c == chips - 1
        if last:
            x_copy(0).start()

        def step(k, _):
            t = c * tiles + k

            @pl.when(t + O_SLOTS - 1 < steps)
            def _():
                w_copy(t + O_SLOTS - 1).start()

            if last:
                @pl.when(k + 1 < tiles)
                def _():
                    x_copy(k + 1).start()

                @pl.when(k >= 2)
                def _():
                    y_copy(k - 2).wait()

                x_copy(k).wait()
            w_copy(t).wait()
            a = jnp.concatenate([got_s[at * 2 * heads + i] for i in range(2 * heads)], axis=1)
            part = _dot(a, w_s[lax.rem(t, O_SLOTS)])
            if c == 0:
                acc_s[k] = part
            elif not last:
                acc_s[k] = acc_s[k] + part
            else:
                y_s[lax.rem(k, 2)] = (x_s[lax.rem(k, 2)].astype(jnp.float32) + (acc_s[k] + part)).astype(jnp.bfloat16)
                y_copy(k).start()

        lax.fori_loop(0, tiles, step, None)
    y_copy(tiles - 2).wait()
    y_copy(tiles - 1).wait()
    for j in range(n - 1):
        send(j, 0).wait_send()


def attend(n, qkv, x, wo):
    _, heads, tokens, _ = qkv.shape
    own, width = x.shape
    tiles = wo.shape[1] // OUT_TILE
    depth = 2 * heads * HEAD
    order = [4, 2, 6, 3, 5, 1, 7, 0] if n == 8 else [*range(1, n), 0]
    hbm = pl.BlockSpec(memory_space=pl.ANY)
    return pl.pallas_call(
        functools.partial(_attend, n, order),
        out_shape=jax.ShapeDtypeStruct(x.shape, jnp.bfloat16),
        in_specs=[hbm, hbm, hbm],
        out_specs=hbm,
        scratch_shapes=[
            pltpu.VMEM(qkv.shape, jnp.bfloat16),
            pltpu.VMEM((n * heads, own, HEAD), jnp.bfloat16),
            pltpu.VMEM((tiles, own, OUT_TILE), jnp.float32),
            pltpu.VMEM((O_SLOTS, depth, OUT_TILE), jnp.bfloat16),
            pltpu.VMEM((heads, own), jnp.float32),
            pltpu.VMEM((heads, HEAD + 8, own), jnp.float32),
            pltpu.VMEM((2, own, OUT_TILE), jnp.bfloat16),
            pltpu.VMEM((2, own, OUT_TILE), jnp.bfloat16),
            pltpu.SemaphoreType.DMA,
            pltpu.SemaphoreType.DMA((O_SLOTS,)),
            pltpu.SemaphoreType.DMA((n - 1,)),
            pltpu.SemaphoreType.DMA((n,)),
            pltpu.SemaphoreType.DMA((2,)),
            pltpu.SemaphoreType.DMA((2,)),
        ],
        compiler_params=pltpu.CompilerParams(collective_id=1, has_side_effects=True, vmem_limit_bytes=VMEM),
        name="attend",
    )(qkv, x, wo)


def solution(mesh):
    n = mesh.shape["sp"]

    def step(x, gain, wq, wk, wv, wo):
        own = x.shape[0]
        half = HEAD // 2
        place = lax.axis_index("sp") * own + jnp.arange(own)
        angle = place.astype(jnp.float32)[:, None] * THETA ** (-jnp.arange(half, dtype=jnp.float32) / half)
        cos, sin = jnp.cos(angle), jnp.sin(angle)
        qkv = project(n, x, gain[None], jnp.concatenate([cos, cos], 1), jnp.concatenate([-sin, sin], 1), wq, wk, wv)
        return attend(n, qkv, x, wo)

    tokens, whole = P(("dp", "sp"), None), P(None, None)
    return jax.shard_map(
        step,
        mesh=mesh,
        in_specs=(tokens, P(None), whole, whole, whole, whole),
        out_specs=tokens,
        check_vma=False,
    )
```

```python
import functools

import jax
import jax.numpy as jnp
from jax import lax
from jax.experimental import pallas as pl
from jax.experimental.pallas import tpu as pltpu
from jax.sharding import PartitionSpec as P

HIDDEN = -2e30
LOG2E = 1.4426950408889634
HEAD = 128
THETA = 10000
MESH = pl.DeviceIdType.MESH
VMEM = 63 * 2**20

TILE_HEADS = 4
W_SLOTS = 3
S_SLOTS = 8
R_SLOTS = 3
G_SLOTS = 3


def _dot(a, b, ca=1, cb=0):
    return lax.dot_general(a, b, (((ca,), (cb,)), ((), ())), preferred_element_type=jnp.float32)


def _kernel(n, x_ref, gain_ref, cos_ref, sin_ref, wq_ref, wk_ref, wv_ref, wo_ref, y_ref,
            a_s, w_s, part_s, out_s, qkv_s, res_s, got_s, acc_s, s_s, p_s, values_s,
            x_sem, w_sem, s_sem, r_sem, o_sem, g_sem, y_sem):
    me = lax.axis_index("sp")
    own, width = x_ref.shape
    cols = TILE_HEADS * HEAD
    halves = n // TILE_HEADS
    per = 3 * halves
    heads = wq_ref.shape[1] // HEAD // n
    group = n * HEAD
    subs = width // group
    rounds = width // cols // subs
    weights = (wq_ref, wk_ref, wv_ref)
    early = 2 * per
    both = per + rounds
    total = heads * both
    e = HEAD**-0.5 * LOG2E

    def w_slot(g):
        return lax.rem(g, W_SLOTS)

    def fetch_tile(g, i, r):
        at = pl.multiple_of((i * halves + lax.rem(r, halves)) * cols, cols)
        for m, w in enumerate(weights):
            @pl.when(lax.div(r, halves) == m)
            def _():
                pltpu.make_async_copy(w.at[:, pl.ds(at, cols)], w_s.at[w_slot(g)], w_sem.at[w_slot(g)]).start()

    def fetch_rows(g, i, r):
        row = pl.multiple_of(i * group, group)
        for b in range(subs):
            at = pl.multiple_of((r * subs + b) * cols, cols)
            pltpu.make_async_copy(wo_ref.at[pl.ds(row, group), pl.ds(at, cols)], w_s.at[w_slot(g), pl.ds(b * group, group), :], w_sem.at[w_slot(g)]).start()

    def fetch(g):
        u, v = g - early, g - early - (heads - 2) * both
        ui, ur = lax.div(u, both), lax.rem(u, both)

        @pl.when(g < early)
        def _():
            fetch_tile(g, lax.div(g, per), lax.rem(g, per))

        @pl.when((u >= 0) & (v < 0))
        def _():
            @pl.when(ur < per)
            def _():
                fetch_tile(g, ui + 2, ur)

            @pl.when(ur >= per)
            def _():
                fetch_rows(g, ui, ur - per)

        @pl.when((v >= 0) & (g < total))
        def _():
            fetch_rows(g, heads - 2 + lax.div(v, rounds), lax.rem(v, rounds))

    def fetched(g):
        pltpu.make_async_copy(wq_ref.at[:, pl.ds(0, cols)], w_s.at[w_slot(g)], w_sem.at[w_slot(g)]).wait()

    def parts(t):
        i, r = lax.div(t, per), lax.rem(t, per)
        return i, lax.div(r, halves), lax.rem(r, halves)

    def q_copy(t, h):
        i, m, half = parts(t)
        slot = lax.rem(t, S_SLOTS)
        to = half * TILE_HEADS + h
        keep = lax.rem(i, R_SLOTS)
        rows = pl.ds(pl.multiple_of(me * own, own), own)
        return to, slot, keep, m, rows, pltpu.make_async_remote_copy(
            src_ref=out_s.at[slot, h], dst_ref=qkv_s.at[keep, m, rows, :], send_sem=s_sem.at[slot, h], recv_sem=r_sem.at[keep, me],
            device_id={"sp": to}, device_id_type=MESH)

    def send(t):
        for h in range(TILE_HEADS):
            to, slot, keep, m, rows, copy = q_copy(t, h)

            @pl.when(to == me)
            def _():
                qkv_s[keep, m, rows, :] = out_s[slot, h]

            @pl.when(to != me)
            def _():
                copy.start()

    def sent(t):
        for h in range(TILE_HEADS):
            to, *_, copy = q_copy(t, h)

            @pl.when(to != me)
            def _():
                copy.wait_send()

    def finish(t):
        _, m, _ = parts(t)
        prev, slot = lax.rem(t + 2, 2), lax.rem(t + S_SLOTS, S_SLOTS)
        for h in range(TILE_HEADS):
            b = part_s[prev, :, h * HEAD : (h + 1) * HEAD].astype(jnp.bfloat16).astype(jnp.float32)
            turned = b * cos_ref[...] + pltpu.roll(b, HEAD // 2, 1) * sin_ref[...]
            out_s[slot, h] = jnp.where(m == 2, b, turned).astype(jnp.bfloat16)

    def r_copy(i, iq):
        slot = lax.rem(i, G_SLOTS)
        return pltpu.make_async_remote_copy(src_ref=res_s.at[slot, iq], dst_ref=got_s.at[slot, me], send_sem=o_sem.at[slot, iq],
                                            recv_sem=g_sem.at[slot, me], device_id={"sp": iq}, device_id_type=MESH)

    def attention(i):
        keep, slot = lax.rem(i, R_SLOTS), lax.rem(i, G_SLOTS)
        for d in range(1, n):
            src = lax.rem(me + d, n)
            block = qkv_s.at[keep, :, pl.ds(pl.multiple_of(src * own, own), own), :]
            pltpu.make_async_copy(block, block, r_sem.at[keep, src]).wait()

        @pl.when(i >= G_SLOTS)
        def _():
            for d in range(1, n):
                r_copy(i - G_SLOTS, lax.rem(me + d, n)).wait_send()

        values_s[:HEAD, :] = qkv_s[keep, 2].T
        values_s[HEAD:, :] = jnp.ones((8, n * own), jnp.bfloat16)
        ok = lax.broadcasted_iota(jnp.int32, (own, own), 1) >= lax.broadcasted_iota(jnp.int32, (own, own), 0)

        def scores(iq):
            top = None
            for c in range(iq + 1):
                s = _dot(qkv_s[keep, 1, c * own : (c + 1) * own, :], qkv_s[keep, 0, iq * own : (iq + 1) * own, :], 1, 1)
                if c == iq:
                    s = jnp.where(ok, s, HIDDEN)
                s_s[iq % 2, c * own : (c + 1) * own, :] = s
                m = s.reshape(own // 8, 8, own).max(axis=0)
                top = m if top is None else jnp.maximum(top, m)
            return top.max(axis=0, keepdims=True)

        top = scores(0)
        for iq in range(n):
            seen = (iq + 1) * own
            later = scores(iq + 1) if iq + 1 < n else None
            for c in range(iq + 1):
                here = slice(c * own, (c + 1) * own)
                p_s[iq % 2, here, :] = jnp.exp2((s_s[iq % 2, here, :] - top) * e).astype(jnp.bfloat16)
            mix = _dot(values_s[:, :seen], p_s[iq % 2, :seen, :])
            res_s[slot, iq] = (mix[:HEAD] * (1 / mix[HEAD : HEAD + 1])).T.astype(jnp.bfloat16)
            top = later
        got_s[slot, me] = res_s[slot, me]
        for d in (4, 2, 6, 3, 5, 1, 7) if n == 8 else range(1, n):
            r_copy(i, lax.rem(me + d, n)).start()

    def project(i, g, last):
        slot = lax.rem(i, G_SLOTS)
        for d in range(1, n):
            src = lax.rem(me + d, n)
            block = got_s.at[slot, src]
            pltpu.make_async_copy(block, block, g_sem.at[slot, src]).wait()

        def one(r, _):
            fetch(g + r + W_SLOTS - 1)
            fetched(g + r)
            a = jnp.concatenate([got_s[slot, s] for s in range(n)], axis=1)
            for b in range(subs):
                y = acc_s[r * subs + b] + _dot(a, w_s[w_slot(g + r), b * group : (b + 1) * group, :])
                if last:
                    a_s[:, pl.ds(pl.multiple_of((r * subs + b) * cols, cols), cols)] = y.astype(jnp.bfloat16)
                else:
                    acc_s[r * subs + b] = y
            if last:
                y_copy(r).start()

        lax.fori_loop(0, rounds, one, None)

    def y_copy(r):
        here = pl.ds(pl.multiple_of(r * subs * cols, subs * cols), subs * cols)
        return pltpu.make_async_copy(a_s.at[:, here], y_ref.at[:, here], y_sem.at[r])

    load = pltpu.make_async_copy(x_ref, a_s, x_sem)
    load.start()
    for g in range(W_SLOTS - 1):
        fetch_tile(g, 0, g)
    load.wait()

    def norm(i, _):
        rows = pl.ds(pl.multiple_of(i * 16, 16), 16)
        wide = a_s[rows, :].astype(jnp.float32)
        scale = lax.rsqrt(jnp.sum(wide * wide, -1, keepdims=True) * (1 / width) + 1e-6)
        for b in range(width // cols):
            here = slice(b * cols, (b + 1) * cols)
            acc_s[b, rows, :] = wide[:, here]
            a_s[rows, here] = (wide[:, here] * scale * gain_ref[here][None].astype(jnp.float32)).astype(jnp.bfloat16)

    lax.fori_loop(0, own // 16, norm, None)
    barrier = pltpu.get_barrier_semaphore()
    for d in range(1, n):
        pl.semaphore_signal(barrier, inc=1, device_id={"sp": lax.rem(me + d, n)}, device_id_type=MESH)
    pl.semaphore_wait(barrier, n - 1)

    def step(i, _):
        start = jnp.where(i < 2, i * per, early + (i - 2) * both)

        def tile(r, _):
            g, t = start + r, i * per + r
            fetch(g + W_SLOTS - 1)

            @pl.when(t >= 2)
            def _():
                send(t - 2)

            @pl.when(t - 1 >= S_SLOTS)
            def _():
                sent(t - 1 - S_SLOTS)

            fetched(g)
            finish(t - 1)
            part_s[lax.rem(t, 2)] = _dot(a_s[...], w_s[w_slot(g)])

        @pl.when(i < heads)
        def _():
            lax.fori_loop(0, per, tile, None)

        @pl.when(i == heads - 1)
        def _():
            t = heads * per
            send(t - 2)
            sent(t - 1 - S_SLOTS)
            finish(t - 1)
            send(t - 1)

        @pl.when((i >= 1) & (i <= heads))
        def _():
            attention(i - 1)

        first = jnp.where(i < heads, start + per, total - (heads + 2 - i) * rounds)

        @pl.when((i >= 2) & (i <= heads))
        def _():
            project(i - 2, first, False)

        @pl.when(i == heads + 1)
        def _():
            project(i - 2, first, True)

    lax.fori_loop(0, heads + 2, step, None)
    lax.fori_loop(heads * per - S_SLOTS, heads * per, lambda t, _: sent(t), None)
    for i in range(heads - G_SLOTS, heads):
        for d in range(1, n):
            r_copy(i, lax.rem(me + d, n)).wait_send()
    for r in range(rounds):
        y_copy(r).wait()


def block(n, x, gain, cos, sin, wq, wk, wv, wo):
    own, width = x.shape
    cols = TILE_HEADS * HEAD
    rounds = width // cols // (width // (n * HEAD))
    vm, hbm = pl.BlockSpec(memory_space=pltpu.VMEM), pl.BlockSpec(memory_space=pl.ANY)
    low = jnp.bfloat16
    return pl.pallas_call(
        functools.partial(_kernel, n),
        out_shape=jax.ShapeDtypeStruct(x.shape, low),
        in_specs=[hbm, vm, vm, vm, hbm, hbm, hbm, hbm],
        out_specs=hbm,
        scratch_shapes=[
            pltpu.VMEM((own, width), low),
            pltpu.VMEM((W_SLOTS, width, cols), low),
            pltpu.VMEM((2, own, cols), jnp.float32),
            pltpu.VMEM((S_SLOTS, TILE_HEADS, own, HEAD), low),
            pltpu.VMEM((R_SLOTS, 3, n * own, HEAD), low),
            pltpu.VMEM((G_SLOTS, n, own, HEAD), low),
            pltpu.VMEM((G_SLOTS, n, own, HEAD), low),
            pltpu.VMEM((width // cols, own, cols), jnp.float32),
            pltpu.VMEM((2, n * own, own), jnp.float32),
            pltpu.VMEM((2, n * own, own), low),
            pltpu.VMEM((HEAD + 8, n * own), low),
            pltpu.SemaphoreType.DMA,
            pltpu.SemaphoreType.DMA((W_SLOTS,)),
            pltpu.SemaphoreType.DMA((S_SLOTS, TILE_HEADS)),
            pltpu.SemaphoreType.DMA((R_SLOTS, n)),
            pltpu.SemaphoreType.DMA((G_SLOTS, n)),
            pltpu.SemaphoreType.DMA((G_SLOTS, n)),
            pltpu.SemaphoreType.DMA((rounds,)),
        ],
        compiler_params=pltpu.CompilerParams(collective_id=0, has_side_effects=True, vmem_limit_bytes=VMEM),
        name="attention_block",
    )(x, gain, cos, sin, wq, wk, wv, wo)


def solution(mesh):
    n = mesh.shape["sp"]

    def step(x, gain, wq, wk, wv, wo):
        own = x.shape[0]
        half = HEAD // 2
        place = lax.axis_index("sp") * own + jnp.arange(own)
        lane = jnp.arange(HEAD)
        angle = place.astype(jnp.float32)[:, None] * THETA ** (-(lane % half).astype(jnp.float32) / half)
        return block(n, x, gain, jnp.cos(angle), jnp.sin(angle) * jnp.where(lane < half, -1.0, 1.0), wq, wk, wv, wo)

    tokens, whole = P(("dp", "sp"), None), P(None, None)
    return jax.shard_map(
        step,
        mesh=mesh,
        in_specs=(tokens, P(None), whole, whole, whole, whole),
        out_specs=tokens,
        check_vma=False,
    )
```

```python
import functools

import jax
import jax.numpy as jnp
from jax import lax
from jax.experimental import pallas as pl
from jax.experimental.pallas import tpu as pltpu
from jax.sharding import PartitionSpec as P

HIDDEN = -2e30
LOG2E = 1.4426950408889634
HEAD = 128
THETA = 10000
MESH = pl.DeviceIdType.MESH
VMEM = 63 * 2**20

TILE_HEADS = 4
W_SLOTS = 3
S_SLOTS = 8
R_SLOTS = 3
G_SLOTS = 4
O_SLOTS = 2
LAG = 3


def _dot(a, b, ca=1, cb=0):
    return lax.dot_general(a, b, (((ca,), (cb,)), ((), ())), preferred_element_type=jnp.float32)


def _kernel(n, x_ref, gain_ref, cos_ref, sin_ref, wq_ref, wk_ref, wv_ref, wo_ref, y_ref,
            a_s, w_s, part_s, out_s, qkv_s, res_s, got_s, acc_s, s_s, p_s, values_s,
            x_sem, w_sem, s_sem, r_sem, o_sem, g_sem, y_sem):
    me = lax.axis_index("sp")
    own, width = x_ref.shape
    cols = TILE_HEADS * HEAD
    halves = n // TILE_HEADS
    per = 3 * halves
    heads = wq_ref.shape[1] // HEAD // n
    group = n * HEAD
    subs = width // group
    rounds = width // cols // subs
    weights = (wq_ref, wk_ref, wv_ref)
    early = LAG * per
    both = per + rounds
    total = heads * both
    e = HEAD**-0.5 * LOG2E

    def w_slot(g):
        return lax.rem(g, W_SLOTS)

    def fetch_tile(g, i, r):
        at = pl.multiple_of((i * halves + lax.rem(r, halves)) * cols, cols)
        for m, w in enumerate(weights):
            @pl.when(lax.div(r, halves) == m)
            def _():
                pltpu.make_async_copy(w.at[:, pl.ds(at, cols)], w_s.at[w_slot(g)], w_sem.at[w_slot(g)]).start(priority=1)

    def fetch_rows(g, i, r):
        row = pl.multiple_of(i * group, group)
        for b in range(subs):
            at = pl.multiple_of((r * subs + b) * cols, cols)
            pltpu.make_async_copy(wo_ref.at[pl.ds(row, group), pl.ds(at, cols)], w_s.at[w_slot(g), pl.ds(b * group, group), :], w_sem.at[w_slot(g)]).start(priority=1)

    def fetch(g):
        u, v = g - early, g - early - (heads - LAG) * both
        ui, ur = lax.div(u, both), lax.rem(u, both)

        @pl.when(g < early)
        def _():
            fetch_tile(g, lax.div(g, per), lax.rem(g, per))

        @pl.when((u >= 0) & (v < 0))
        def _():
            @pl.when(ur < per)
            def _():
                fetch_tile(g, ui + LAG, ur)

            @pl.when(ur >= per)
            def _():
                fetch_rows(g, ui, ur - per)

        @pl.when((v >= 0) & (g < total))
        def _():
            fetch_rows(g, heads - LAG + lax.div(v, rounds), lax.rem(v, rounds))

    def fetched(g):
        pltpu.make_async_copy(wq_ref.at[:, pl.ds(0, cols)], w_s.at[w_slot(g)], w_sem.at[w_slot(g)]).wait()

    def parts(t):
        i, r = lax.div(t, per), lax.rem(t, per)
        return i, lax.div(r, halves), lax.rem(r, halves)

    def q_copy(t, h):
        i, m, half = parts(t)
        slot = lax.rem(t, S_SLOTS)
        to = half * TILE_HEADS + h
        keep = lax.rem(i, R_SLOTS)
        rows = pl.ds(pl.multiple_of(me * own, own), own)
        return to, slot, keep, m, rows, pltpu.make_async_remote_copy(
            src_ref=out_s.at[slot, h], dst_ref=qkv_s.at[keep, m, rows, :], send_sem=s_sem.at[slot, h], recv_sem=r_sem.at[keep, me],
            device_id={"sp": to}, device_id_type=MESH)

    def send(t):
        for h in range(TILE_HEADS):
            to, slot, keep, m, rows, copy = q_copy(t, h)

            @pl.when(to == me)
            def _():
                qkv_s[keep, m, rows, :] = out_s[slot, h]

            @pl.when(to != me)
            def _():
                copy.start()

    def sent(t):
        for h in range(TILE_HEADS):
            to, *_, copy = q_copy(t, h)

            @pl.when(to != me)
            def _():
                copy.wait_send()

    def finish(t):
        _, m, _ = parts(t)
        prev, slot = lax.rem(t + 2, 2), lax.rem(t + S_SLOTS, S_SLOTS)
        for h in range(TILE_HEADS):
            b = part_s[prev, :, h * HEAD : (h + 1) * HEAD].astype(jnp.bfloat16).astype(jnp.float32)
            turned = b * cos_ref[...] + pltpu.roll(b, HEAD // 2, 1) * sin_ref[...]
            out_s[slot, h] = jnp.where(m == 2, b, turned).astype(jnp.bfloat16)

    def r_copy(i, iq):
        own_slot, slot = lax.rem(i, O_SLOTS), lax.rem(i, G_SLOTS)
        return pltpu.make_async_remote_copy(src_ref=res_s.at[own_slot, iq], dst_ref=got_s.at[slot, me], send_sem=o_sem.at[own_slot, iq],
                                            recv_sem=g_sem.at[slot, me], device_id={"sp": iq}, device_id_type=MESH)

    def attention(i):
        keep, slot = lax.rem(i, R_SLOTS), lax.rem(i, O_SLOTS)
        for d in range(1, n):
            src = lax.rem(me + d, n)
            block = qkv_s.at[keep, :, pl.ds(pl.multiple_of(src * own, own), own), :]
            pltpu.make_async_copy(block, block, r_sem.at[keep, src]).wait()

        @pl.when(i >= O_SLOTS)
        def _():
            for d in range(1, n):
                r_copy(i - O_SLOTS, lax.rem(me + d, n)).wait_send()

        values_s[:HEAD, :] = qkv_s[keep, 2].T
        values_s[HEAD:, :] = jnp.ones((8, n * own), jnp.bfloat16)
        ok = lax.broadcasted_iota(jnp.int32, (own, own), 1) >= lax.broadcasted_iota(jnp.int32, (own, own), 0)

        def scores(iq):
            top = None
            for c in range(iq + 1):
                s = _dot(qkv_s[keep, 1, c * own : (c + 1) * own, :], qkv_s[keep, 0, iq * own : (iq + 1) * own, :], 1, 1)
                if c == iq:
                    s = jnp.where(ok, s, HIDDEN)
                s_s[iq % 2, c * own : (c + 1) * own, :] = s
                m = s.reshape(own // 8, 8, own).max(axis=0)
                top = m if top is None else jnp.maximum(top, m)
            return top.max(axis=0, keepdims=True)

        top = scores(0)
        for iq in range(n):
            seen = (iq + 1) * own
            later = scores(iq + 1) if iq + 1 < n else None
            for c in range(iq + 1):
                here = slice(c * own, (c + 1) * own)
                p_s[iq % 2, here, :] = jnp.exp2((s_s[iq % 2, here, :] - top) * e).astype(jnp.bfloat16)
            mix = _dot(values_s[:, :seen], p_s[iq % 2, :seen, :])
            res_s[slot, iq] = (mix[:HEAD] * (1 / mix[HEAD : HEAD + 1])).T.astype(jnp.bfloat16)
            top = later
        got_s[lax.rem(i, G_SLOTS), me] = res_s[slot, me]
        for d in (4, 2, 6, 3, 5, 1, 7) if n == 8 else range(1, n):
            r_copy(i, lax.rem(me + d, n)).start()

    def project(i, g, last):
        slot = lax.rem(i, G_SLOTS)
        for d in range(1, n):
            src = lax.rem(me + d, n)
            block = got_s.at[slot, src]
            pltpu.make_async_copy(block, block, g_sem.at[slot, src]).wait()

        def one(r, _):
            fetch(g + r + W_SLOTS - 1)
            fetched(g + r)
            a = jnp.concatenate([got_s[slot, s] for s in range(n)], axis=1)
            for b in range(subs):
                y = acc_s[r * subs + b] + _dot(a, w_s[w_slot(g + r), b * group : (b + 1) * group, :])
                if last:
                    a_s[:, pl.ds(pl.multiple_of((r * subs + b) * cols, cols), cols)] = y.astype(jnp.bfloat16)
                else:
                    acc_s[r * subs + b] = y
            if last:
                y_copy(r).start()

        lax.fori_loop(0, rounds, one, None)

    def y_copy(r):
        here = pl.ds(pl.multiple_of(r * subs * cols, subs * cols), subs * cols)
        return pltpu.make_async_copy(a_s.at[:, here], y_ref.at[:, here], y_sem.at[r])

    load = pltpu.make_async_copy(x_ref, a_s, x_sem)
    load.start()
    load.wait()
    for g in range(W_SLOTS - 1):
        fetch_tile(g, 0, g)

    def norm(i, _):
        rows = pl.ds(pl.multiple_of(i * 16, 16), 16)
        squares = jnp.zeros((16, HEAD), jnp.float32)
        for b in range(width // cols):
            wide = a_s[rows, b * cols : (b + 1) * cols].astype(jnp.float32)
            acc_s[b, rows, :] = wide
            for h in range(TILE_HEADS):
                one = wide[:, h * HEAD : (h + 1) * HEAD]
                squares = squares + one * one
        scale = lax.rsqrt(jnp.sum(squares, -1, keepdims=True) * (1 / width) + 1e-6)
        for b in range(width // cols):
            here = slice(b * cols, (b + 1) * cols)
            a_s[rows, here] = (acc_s[b, rows, :] * scale * gain_ref[here][None].astype(jnp.float32)).astype(jnp.bfloat16)

    lax.fori_loop(0, own // 16, norm, None)
    barrier = pltpu.get_barrier_semaphore()
    for d in range(1, n):
        pl.semaphore_signal(barrier, inc=1, device_id={"sp": lax.rem(me + d, n)}, device_id_type=MESH)
    pl.semaphore_wait(barrier, n - 1)

    def step(i, _):
        start = jnp.where(i < LAG, i * per, early + (i - LAG) * both)

        def tile(r, _):
            g, t = start + r, i * per + r
            fetch(g + W_SLOTS - 1)

            @pl.when(t >= 2)
            def _():
                send(t - 2)

            @pl.when(t - 1 >= S_SLOTS)
            def _():
                sent(t - 1 - S_SLOTS)

            fetched(g)
            finish(t - 1)
            part_s[lax.rem(t, 2)] = _dot(a_s[...], w_s[w_slot(g)])

        @pl.when(i < heads)
        def _():
            lax.fori_loop(0, per, tile, None)

        @pl.when(i == heads - 1)
        def _():
            t = heads * per
            send(t - 2)
            sent(t - 1 - S_SLOTS)
            finish(t - 1)
            send(t - 1)

        @pl.when((i >= 1) & (i <= heads))
        def _():
            attention(i - 1)

        first = jnp.where(i < heads, start + per, total - (heads + LAG - i) * rounds)

        @pl.when((i >= LAG) & (i <= heads + LAG - 2))
        def _():
            project(i - LAG, first, False)

        @pl.when(i == heads + LAG - 1)
        def _():
            project(i - LAG, first, True)

    lax.fori_loop(0, heads + LAG, step, None)
    lax.fori_loop(heads * per - S_SLOTS, heads * per, lambda t, _: sent(t), None)
    for i in range(heads - O_SLOTS, heads):
        for d in range(1, n):
            r_copy(i, lax.rem(me + d, n)).wait_send()
    for r in range(rounds):
        y_copy(r).wait()


def block(n, x, gain, cos, sin, wq, wk, wv, wo):
    own, width = x.shape
    cols = TILE_HEADS * HEAD
    rounds = width // cols // (width // (n * HEAD))
    vm, hbm = pl.BlockSpec(memory_space=pltpu.VMEM), pl.BlockSpec(memory_space=pl.ANY)
    low = jnp.bfloat16
    return pl.pallas_call(
        functools.partial(_kernel, n),
        out_shape=jax.ShapeDtypeStruct(x.shape, low),
        in_specs=[hbm, vm, vm, vm, hbm, hbm, hbm, hbm],
        out_specs=hbm,
        scratch_shapes=[
            pltpu.VMEM((own, width), low),
            pltpu.VMEM((W_SLOTS, width, cols), low),
            pltpu.VMEM((2, own, cols), jnp.float32),
            pltpu.VMEM((S_SLOTS, TILE_HEADS, own, HEAD), low),
            pltpu.VMEM((R_SLOTS, 3, n * own, HEAD), low),
            pltpu.VMEM((O_SLOTS, n, own, HEAD), low),
            pltpu.VMEM((G_SLOTS, n, own, HEAD), low),
            pltpu.VMEM((width // cols, own, cols), jnp.float32),
            pltpu.VMEM((2, n * own, own), jnp.float32),
            pltpu.VMEM((2, n * own, own), low),
            pltpu.VMEM((HEAD + 8, n * own), low),
            pltpu.SemaphoreType.DMA,
            pltpu.SemaphoreType.DMA((W_SLOTS,)),
            pltpu.SemaphoreType.DMA((S_SLOTS, TILE_HEADS)),
            pltpu.SemaphoreType.DMA((R_SLOTS, n)),
            pltpu.SemaphoreType.DMA((O_SLOTS, n)),
            pltpu.SemaphoreType.DMA((G_SLOTS, n)),
            pltpu.SemaphoreType.DMA((rounds,)),
        ],
        compiler_params=pltpu.CompilerParams(collective_id=0, has_side_effects=True, vmem_limit_bytes=VMEM),
        name="attention_block",
    )(x, gain, cos, sin, wq, wk, wv, wo)


def solution(mesh):
    n = mesh.shape["sp"]

    def step(x, gain, wq, wk, wv, wo):
        own = x.shape[0]
        half = HEAD // 2
        place = lax.axis_index("sp") * own + jnp.arange(own)
        lane = jnp.arange(HEAD)
        angle = place.astype(jnp.float32)[:, None] * THETA ** (-(lane % half).astype(jnp.float32) / half)
        return block(n, x, gain, jnp.cos(angle), jnp.sin(angle) * jnp.where(lane < half, -1.0, 1.0), wq, wk, wv, wo)

    tokens, whole = P(("dp", "sp"), None), P(None, None)
    return jax.shard_map(
        step,
        mesh=mesh,
        in_specs=(tokens, P(None), whole, whole, whole, whole),
        out_specs=tokens,
        check_vma=False,
    )
```

```python
import functools

import jax
import jax.numpy as jnp
from jax import lax
from jax.experimental import pallas as pl
from jax.experimental.pallas import tpu as pltpu
from jax.sharding import PartitionSpec as P

HIDDEN = -2e30
LOG2E = 1.4426950408889634
HEAD = 128
THETA = 10000
MESH = pl.DeviceIdType.MESH
VMEM = 63 * 2**20

TILE_HEADS = 4
W_SLOTS = 3
S_SLOTS = 8
R_SLOTS = 3
G_SLOTS = 4
O_SLOTS = 2
LAG = 3


def _dot(a, b, ca=1, cb=0):
    return lax.dot_general(a, b, (((ca,), (cb,)), ((), ())), preferred_element_type=jnp.float32)


def _kernel(n, x_ref, gain_ref, cos_ref, sin_ref, wq_ref, wk_ref, wv_ref, wo_ref, y_ref,
            a_s, w_s, part_s, out_s, qkv_s, res_s, got_s, acc_s, s_s, p_s, values_s,
            x_sem, w_sem, s_sem, r_sem, o_sem, g_sem, y_sem):
    me = lax.axis_index("sp")
    own, width = x_ref.shape
    cols = TILE_HEADS * HEAD
    halves = n // TILE_HEADS
    per = 3 * halves
    heads = wq_ref.shape[1] // HEAD // n
    group = n * HEAD
    subs = width // group
    rounds = width // cols // subs
    weights = (wq_ref, wk_ref, wv_ref)
    early = LAG * per
    both = per + rounds
    total = heads * both
    e = HEAD**-0.5 * LOG2E

    def w_slot(g):
        return lax.rem(g, W_SLOTS)

    def fetch_tile(g, i, r):
        at = pl.multiple_of((i * halves + lax.rem(r, halves)) * cols, cols)
        for m, w in enumerate(weights):
            @pl.when(lax.div(r, halves) == m)
            def _():
                pltpu.make_async_copy(w.at[:, pl.ds(at, cols)], w_s.at[w_slot(g)], w_sem.at[w_slot(g)]).start(priority=1)

    def fetch_rows(g, i, r):
        row = pl.multiple_of(i * group, group)
        for b in range(subs):
            at = pl.multiple_of((r * subs + b) * cols, cols)
            pltpu.make_async_copy(wo_ref.at[pl.ds(row, group), pl.ds(at, cols)], w_s.at[w_slot(g), pl.ds(b * group, group), :], w_sem.at[w_slot(g)]).start(priority=1)

    def fetch(g):
        u, v = g - early, g - early - (heads - LAG) * both
        ui, ur = lax.div(u, both), lax.rem(u, both)

        @pl.when(g < early)
        def _():
            fetch_tile(g, lax.div(g, per), lax.rem(g, per))

        @pl.when((u >= 0) & (v < 0))
        def _():
            @pl.when(ur < per)
            def _():
                fetch_tile(g, ui + LAG, ur)

            @pl.when(ur >= per)
            def _():
                fetch_rows(g, ui, ur - per)

        @pl.when((v >= 0) & (g < total))
        def _():
            fetch_rows(g, heads - LAG + lax.div(v, rounds), lax.rem(v, rounds))

    def fetched(g):
        pltpu.make_async_copy(wq_ref.at[:, pl.ds(0, cols)], w_s.at[w_slot(g)], w_sem.at[w_slot(g)]).wait()

    def parts(t):
        i, r = lax.div(t, per), lax.rem(t, per)
        return i, lax.div(r, halves), lax.rem(r, halves)

    def q_copy(t, h):
        i, m, half = parts(t)
        slot = lax.rem(t, S_SLOTS)
        to = half * TILE_HEADS + h
        keep = lax.rem(i, R_SLOTS)
        rows = pl.ds(pl.multiple_of(me * own, own), own)
        return to, slot, keep, m, rows, pltpu.make_async_remote_copy(
            src_ref=out_s.at[slot, h], dst_ref=qkv_s.at[keep, m, rows, :], send_sem=s_sem.at[slot, h], recv_sem=r_sem.at[keep, me],
            device_id={"sp": to}, device_id_type=MESH)

    def send(t):
        i, m, half = parts(t)
        for h in range(TILE_HEADS):
            to, *_, copy = q_copy(t, h)

            @pl.when(to != me)
            def _():
                copy.start()

        @pl.when(half == lax.div(me, TILE_HEADS))
        def _():
            rows = pl.ds(pl.multiple_of(me * own, own), own)
            qkv_s[lax.rem(i, R_SLOTS), m, rows, :] = out_s[lax.rem(t, S_SLOTS), lax.rem(me, TILE_HEADS)]

    def sent(t):
        for h in range(TILE_HEADS):
            to, *_, copy = q_copy(t, h)

            @pl.when(to != me)
            def _():
                copy.wait_send()

    def finish(t):
        _, m, _ = parts(t)
        prev, slot = lax.rem(t + 2, 2), lax.rem(t + S_SLOTS, S_SLOTS)
        for h in range(TILE_HEADS):
            b = part_s[prev, :, h * HEAD : (h + 1) * HEAD].astype(jnp.bfloat16).astype(jnp.float32)
            turned = b * cos_ref[...] + pltpu.roll(b, HEAD // 2, 1) * sin_ref[...]
            out_s[slot, h] = jnp.where(m == 2, b, turned).astype(jnp.bfloat16)

    def r_copy(i, iq):
        own_slot, slot = lax.rem(i, O_SLOTS), lax.rem(i, G_SLOTS)
        return pltpu.make_async_remote_copy(src_ref=res_s.at[own_slot, iq], dst_ref=got_s.at[slot, me], send_sem=o_sem.at[own_slot, iq],
                                            recv_sem=g_sem.at[slot, me], device_id={"sp": iq}, device_id_type=MESH)

    def attention(i):
        keep, slot = lax.rem(i, R_SLOTS), lax.rem(i, O_SLOTS)
        for d in range(1, n):
            src = lax.rem(me + d, n)
            block = qkv_s.at[keep, :, pl.ds(pl.multiple_of(src * own, own), own), :]
            pltpu.make_async_copy(block, block, r_sem.at[keep, src]).wait()

        @pl.when(i >= O_SLOTS)
        def _():
            for d in range(1, n):
                r_copy(i - O_SLOTS, lax.rem(me + d, n)).wait_send()

        values_s[:HEAD, :] = qkv_s[keep, 2].T
        values_s[HEAD:, :] = jnp.ones((8, n * own), jnp.bfloat16)
        ok = lax.broadcasted_iota(jnp.int32, (own, own), 1) >= lax.broadcasted_iota(jnp.int32, (own, own), 0)

        def scores(iq):
            top = None
            for c in range(iq + 1):
                s = _dot(qkv_s[keep, 1, c * own : (c + 1) * own, :], qkv_s[keep, 0, iq * own : (iq + 1) * own, :], 1, 1)
                if c == iq:
                    s = jnp.where(ok, s, HIDDEN)
                s_s[iq % 2, c * own : (c + 1) * own, :] = s
                m = s.reshape(own // 8, 8, own).max(axis=0)
                top = m if top is None else jnp.maximum(top, m)
            return top.max(axis=0, keepdims=True)

        top = scores(0)
        for iq in range(n + 1):
            later = scores(iq + 1) if iq + 1 < n else None
            if iq < n:
                for c in range(iq + 1):
                    here = slice(c * own, (c + 1) * own)
                    p_s[iq % 2, here, :] = jnp.exp2((s_s[iq % 2, here, :] - top) * e).astype(jnp.bfloat16)
            if iq >= 1:
                seen = iq * own
                mix = _dot(values_s[:, :seen], p_s[(iq - 1) % 2, :seen, :])
                res_s[slot, iq - 1] = (mix[:HEAD] * (1 / mix[HEAD : HEAD + 1])).T.astype(jnp.bfloat16)
            top = later
        got_s[lax.rem(i, G_SLOTS), me] = res_s[slot, me]
        for d in (4, 2, 6, 3, 5, 1, 7) if n == 8 else range(1, n):
            r_copy(i, lax.rem(me + d, n)).start()

    def project(i, g, last):
        slot = lax.rem(i, G_SLOTS)
        for d in range(1, n):
            src = lax.rem(me + d, n)
            block = got_s.at[slot, src]
            pltpu.make_async_copy(block, block, g_sem.at[slot, src]).wait()

        def one(r, _):
            fetch(g + r + W_SLOTS - 1)
            fetched(g + r)
            a = jnp.concatenate([got_s[slot, s] for s in range(n)], axis=1)
            for b in range(subs):
                y = acc_s[r * subs + b] + _dot(a, w_s[w_slot(g + r), b * group : (b + 1) * group, :])
                if last:
                    a_s[:, pl.ds(pl.multiple_of((r * subs + b) * cols, cols), cols)] = y.astype(jnp.bfloat16)
                else:
                    acc_s[r * subs + b] = y
            if last:
                y_copy(r).start()

        lax.fori_loop(0, rounds, one, None)

    def y_copy(r):
        here = pl.ds(pl.multiple_of(r * subs * cols, subs * cols), subs * cols)
        return pltpu.make_async_copy(a_s.at[:, here], y_ref.at[:, here], y_sem.at[r])

    load = pltpu.make_async_copy(x_ref, a_s, x_sem)
    load.start()
    load.wait()
    for g in range(W_SLOTS - 1):
        fetch_tile(g, 0, g)

    def norm(i, _):
        rows = pl.ds(pl.multiple_of(i * 16, 16), 16)
        squares = jnp.zeros((16, HEAD), jnp.float32)
        for b in range(width // cols):
            wide = a_s[rows, b * cols : (b + 1) * cols].astype(jnp.float32)
            acc_s[b, rows, :] = wide
            for h in range(TILE_HEADS):
                one = wide[:, h * HEAD : (h + 1) * HEAD]
                squares = squares + one * one
        scale = lax.rsqrt(jnp.sum(squares, -1, keepdims=True) * (1 / width) + 1e-6)
        for b in range(width // cols):
            here = slice(b * cols, (b + 1) * cols)
            a_s[rows, here] = (acc_s[b, rows, :] * scale * gain_ref[here][None].astype(jnp.float32)).astype(jnp.bfloat16)

    lax.fori_loop(0, own // 16, norm, None)
    barrier = pltpu.get_barrier_semaphore()
    for d in range(1, n):
        pl.semaphore_signal(barrier, inc=1, device_id={"sp": lax.rem(me + d, n)}, device_id_type=MESH)
    pl.semaphore_wait(barrier, n - 1)

    def step(i, _):
        start = jnp.where(i < LAG, i * per, early + (i - LAG) * both)

        def tile(r, _):
            g, t = start + r, i * per + r
            fetch(g + W_SLOTS - 1)

            @pl.when(t >= 2)
            def _():
                send(t - 2)

            @pl.when(t - 1 >= S_SLOTS)
            def _():
                sent(t - 1 - S_SLOTS)

            fetched(g)
            finish(t - 1)
            part_s[lax.rem(t, 2)] = _dot(a_s[...], w_s[w_slot(g)])

        @pl.when(i < heads)
        def _():
            lax.fori_loop(0, per, tile, None)

        @pl.when(i == heads - 1)
        def _():
            t = heads * per
            send(t - 2)
            sent(t - 1 - S_SLOTS)
            finish(t - 1)
            send(t - 1)

        @pl.when((i >= 1) & (i <= heads))
        def _():
            attention(i - 1)

        first = jnp.where(i < heads, start + per, total - (heads + LAG - i) * rounds)

        @pl.when((i >= LAG) & (i <= heads + LAG - 2))
        def _():
            project(i - LAG, first, False)

        @pl.when(i == heads + LAG - 1)
        def _():
            project(i - LAG, first, True)

    lax.fori_loop(0, heads + LAG, step, None)
    lax.fori_loop(heads * per - S_SLOTS, heads * per, lambda t, _: sent(t), None)
    for i in range(heads - O_SLOTS, heads):
        for d in range(1, n):
            r_copy(i, lax.rem(me + d, n)).wait_send()
    for r in range(rounds):
        y_copy(r).wait()


def block(n, x, gain, cos, sin, wq, wk, wv, wo):
    own, width = x.shape
    cols = TILE_HEADS * HEAD
    rounds = width // cols // (width // (n * HEAD))
    vm, hbm = pl.BlockSpec(memory_space=pltpu.VMEM), pl.BlockSpec(memory_space=pl.ANY)
    low = jnp.bfloat16
    return pl.pallas_call(
        functools.partial(_kernel, n),
        out_shape=jax.ShapeDtypeStruct(x.shape, low),
        in_specs=[hbm, vm, vm, vm, hbm, hbm, hbm, hbm],
        out_specs=hbm,
        scratch_shapes=[
            pltpu.VMEM((own, width), low),
            pltpu.VMEM((W_SLOTS, width, cols), low),
            pltpu.VMEM((2, own, cols), jnp.float32),
            pltpu.VMEM((S_SLOTS, TILE_HEADS, own, HEAD), low),
            pltpu.VMEM((R_SLOTS, 3, n * own, HEAD), low),
            pltpu.VMEM((O_SLOTS, n, own, HEAD), low),
            pltpu.VMEM((G_SLOTS, n, own, HEAD), low),
            pltpu.VMEM((width // cols, own, cols), jnp.float32),
            pltpu.VMEM((2, n * own, own), jnp.float32),
            pltpu.VMEM((2, n * own, own), low),
            pltpu.VMEM((HEAD + 8, n * own), low),
            pltpu.SemaphoreType.DMA,
            pltpu.SemaphoreType.DMA((W_SLOTS,)),
            pltpu.SemaphoreType.DMA((S_SLOTS, TILE_HEADS)),
            pltpu.SemaphoreType.DMA((R_SLOTS, n)),
            pltpu.SemaphoreType.DMA((O_SLOTS, n)),
            pltpu.SemaphoreType.DMA((G_SLOTS, n)),
            pltpu.SemaphoreType.DMA((rounds,)),
        ],
        compiler_params=pltpu.CompilerParams(collective_id=0, has_side_effects=True, vmem_limit_bytes=VMEM),
        name="attention_block",
    )(x, gain, cos, sin, wq, wk, wv, wo)


def solution(mesh):
    n = mesh.shape["sp"]

    def step(x, gain, wq, wk, wv, wo):
        own = x.shape[0]
        half = HEAD // 2
        place = lax.axis_index("sp") * own + jnp.arange(own)
        lane = jnp.arange(HEAD)
        angle = place.astype(jnp.float32)[:, None] * THETA ** (-(lane % half).astype(jnp.float32) / half)
        return block(n, x, gain, jnp.cos(angle), jnp.sin(angle) * jnp.where(lane < half, -1.0, 1.0), wq, wk, wv, wo)

    tokens, whole = P(("dp", "sp"), None), P(None, None)
    return jax.shard_map(
        step,
        mesh=mesh,
        in_specs=(tokens, P(None), whole, whole, whole, whole),
        out_specs=tokens,
        check_vma=False,
    )
```
